32 devices in a mesh: row: 4 (over y, x), col: 8 (over z, core).
Axes of the slice: x: 2, y: 2, z: 4, core: 2. Of those that a mesh axis runs over, the one named last changes fastest.
Arguments:
- user_feats: bfloat16 [4096, 128], P(('row', 'col')), may hold values from -6 to 6
- item_feats: bfloat16 [16384, 128], P(('col', 'row')), may hold values from -6 to 6
- tile_values: bfloat16 [4, 8, 1, 512, 512], P('row', 'col'), may hold values from -0.15625 to 0.15625
- tile_coords: int32 [4, 8, 2, 1], P('row', 'col'), may hold values from 0 to 3, as said below
- tile_count: int32 [4, 8], P('row', 'col'), may hold values from 1 to 1, as said below
Outputs:
- users_next: bfloat16 [4096, 128], P(('row', 'col'))
- items_next: bfloat16 [16384, 128], P(('col', 'row'))
The draws below stay inside these ranges and needn't reach their ends.
Inputs may be any that keep to these rules, and one draw needn't show every extreme that they name: `tile_coords`: within one device's first tile_count slots the pairs (user tile, item tile) are distinct; the first entry is a user tile below 2, the second an item tile below 4; slots at or after the count carry no tile. `tile_count`: at least one device has all 1 slots live.
All inputs are finite; a program needn't handle non-finite values.
Results may differ from the reference program's by a relative error of at most 0.001.
Values may be sent and summed in bfloat16 or wider, within the bound.
A program may use at most 64 MiB of HBM per device.

```python
import jax
import jax.numpy as jnp
from jax import lax

W = 128
TS = 512
UT = 2
IT = 4
MAXT = 1
USERS = 4096
ITEMS = 16384
N_ROW = 4
N_COL = 8


def draw_tile_coords(key, part):
    keys = jax.random.split(jax.random.fold_in(key, 7), N_ROW * N_COL)
    perms = jax.vmap(lambda single: jax.random.permutation(single, UT * IT))(keys)
    places = perms[:, :MAXT].reshape(N_ROW, N_COL, MAXT).astype(jnp.int32)
    return jnp.stack([places // IT, places % IT], axis=2).astype(jnp.int32)


def draw_tile_count(key, part):
    first, second, third = jax.random.split(jax.random.fold_in(key, 11), 3)
    draw_one = jax.random.randint(first, (N_ROW * N_COL,), 1, MAXT + 1)
    draw_two = jax.random.randint(second, (N_ROW * N_COL,), 1, MAXT + 1)
    counts = jnp.minimum(draw_one, draw_two)
    busiest = jax.random.randint(third, (), 0, N_ROW * N_COL)
    counts = jnp.where(jnp.arange(N_ROW * N_COL) == busiest, MAXT, counts)
    return counts.reshape(N_ROW, N_COL).astype(jnp.int32)


def steps_of(stream_key, dims, cuts, least, largest):
    def one(dim, shards_of):
        steps = jax.random.uniform(jax.random.fold_in(jax.random.fold_in(stream_key, 6), dim), (shards_of,), jnp.float32, least / len(cuts), largest / len(cuts))
        return jnp.repeat(jnp.exp(steps), dims[dim] // shards_of).reshape((-1,) + (1,) * (len(dims) - dim - 1))

    factor_of = one(*cuts[0])
    for cut in cuts[1:]:
        factor_of = factor_of * one(*cut)
    return factor_of


def centred(rng, shape, deviation, bound, shards=(), dtype=jnp.bfloat16):
    loudness = steps_of(rng, shape, shards, -0.22, 0.18) if shards else 1.0
    values = jax.random.normal(rng, shape, jnp.float32) * deviation * loudness
    return jnp.minimum(jnp.maximum(values, -bound), bound).astype(dtype)


def setup_inputs(seed: int = 0) -> dict:
    key_of = jax.random.split(jax.random.key(seed), 6)
    user_feats = centred(key_of[0], (USERS, W), 1.0, 6.0, ((0, 32),))
    item_feats = centred(key_of[1], (ITEMS, W), 1.0, 6.0, ((0, 32),))
    tile_values = centred(key_of[2], (N_ROW, N_COL, MAXT, TS, TS), (3 * TS) ** -0.5, 0.15625, ((0, 4), (1, 8)))
    tile_coords = draw_tile_coords(jax.random.fold_in(key_of[5], 71), 0)
    tile_count = draw_tile_count(jax.random.fold_in(key_of[5], 71), 0)
    return dict(user_feats=user_feats, item_feats=item_feats, tile_values=tile_values, tile_coords=tile_coords, tile_count=tile_count)


def reference(user_feats, item_feats, tile_values, tile_coords, tile_count):
    total = N_ROW * N_COL * MAXT

    def step(index, carry):
        acc_users, acc_items = carry
        index = jnp.asarray(index).astype(jnp.int32)
        device = index // MAXT
        slot = index % MAXT
        row_id = device // N_COL
        col_id = device % N_COL
        tile = tile_values[row_id, col_id, slot]
        user_tile = tile_coords[row_id, col_id, 0, slot].astype(jnp.int32)
        item_tile = tile_coords[row_id, col_id, 1, slot].astype(jnp.int32)
        live = slot < tile_count[row_id, col_id]
        user_start = ((row_id * UT + user_tile) * TS).astype(jnp.int32)
        item_start = ((col_id * IT + item_tile) * TS).astype(jnp.int32)
        item_part = lax.dynamic_slice_in_dim(item_feats, item_start, TS, 0)
        user_part = lax.dynamic_slice_in_dim(user_feats, user_start, TS, 0)
        to_users = jnp.dot(tile, item_part, preferred_element_type=jnp.float32)
        to_items = jnp.dot(tile.T, user_part, preferred_element_type=jnp.float32)
        to_users = jnp.where(live, to_users, jnp.zeros_like(to_users))
        to_items = jnp.where(live, to_items, jnp.zeros_like(to_items))
        old_users = lax.dynamic_slice_in_dim(acc_users, user_start, TS, 0)
        old_items = lax.dynamic_slice_in_dim(acc_items, item_start, TS, 0)
        acc_users = lax.dynamic_update_slice_in_dim(acc_users, old_users + to_users, user_start, 0)
        acc_items = lax.dynamic_update_slice_in_dim(acc_items, old_items + to_items, item_start, 0)
        return acc_users, acc_items

    start = (jnp.zeros((USERS, W), jnp.float32), jnp.zeros((ITEMS, W), jnp.float32))
    acc_users, acc_items = lax.fori_loop(jnp.int32(0), jnp.int32(total), step, start)
    return acc_users.astype(jnp.bfloat16), acc_items.astype(jnp.bfloat16)
```

```python
import functools

import jax
import jax.numpy as jnp
from jax import lax
from jax.experimental import pallas as pl
from jax.experimental.pallas import tpu as pltpu
from jax.sharding import PartitionSpec as P

MESH = pl.DeviceIdType.MESH


def gathered(user_feats, item_feats, tile_values, tile_coords, tile_count):
    user_block = lax.all_gather(user_feats, "col", axis=0, tiled=True)
    item_block = lax.all_gather(item_feats, "row", axis=0, tiled=True)
    tiles = tile_values[0, 0]
    coords = tile_coords[0, 0]
    count = tile_count[0, 0]
    slots = tiles.shape[0]
    size = tiles.shape[1]
    width = user_block.shape[1]
    user_tiles = user_block.shape[0] // size
    item_tiles = item_block.shape[0] // size
    live = jnp.arange(slots) < count
    pick_user = ((coords[0][:, None] == jnp.arange(user_tiles)[None, :]) & live[:, None]).astype(
        jnp.bfloat16
    )
    pick_item = (coords[1][:, None] == jnp.arange(item_tiles)[None, :]).astype(jnp.bfloat16)
    user_sel = jnp.einsum(
        "su,uiw->siw",
        pick_user,
        user_block.reshape(user_tiles, size, width),
        preferred_element_type=jnp.float32,
    ).astype(jnp.bfloat16)
    item_sel = jnp.einsum(
        "st,tjw->sjw",
        pick_item,
        item_block.reshape(item_tiles, size, width),
        preferred_element_type=jnp.float32,
    ).astype(jnp.bfloat16)
    to_users = jnp.einsum("sij,sjw->siw", tiles, item_sel, preferred_element_type=jnp.float32)
    to_items = jnp.einsum("sij,siw->sjw", tiles, user_sel, preferred_element_type=jnp.float32)
    part_users = jnp.einsum(
        "su,siw->uiw", pick_user.astype(jnp.float32), to_users, precision=lax.Precision.HIGHEST
    ).reshape(user_tiles * size, width)
    part_items = jnp.einsum(
        "st,sjw->tjw", pick_item.astype(jnp.float32), to_items, precision=lax.Precision.HIGHEST
    ).reshape(item_tiles * size, width)
    users_next = lax.psum_scatter(part_users, "col", scatter_dimension=0, tiled=True)
    items_next = lax.psum_scatter(part_items, "row", scatter_dimension=0, tiled=True)
    return (users_next.astype(jnp.bfloat16), items_next.astype(jnp.bfloat16))


def kernel(
    n_z,
    coords,
    count,
    user_in,
    item_in,
    tile_in,
    out_u,
    out_i,
    u_all,
    i_all,
    tile_v,
    tile_t,
    meta,
    meta_x,
    meta_y,
    meta_p,
    part_u,
    from_p,
    send_z,
    from_z,
    part_i,
    from_1,
    send_2,
    from_2,
    load_sem,
    meta_s,
    meta_r,
    uz_s,
    uz_r,
    up_s,
    up_r,
    ig_s,
    ig_r,
    rp_s,
    rp_r,
    rz_s,
    rz_r,
    r1_s,
    r1_r,
    r2_s,
    r2_r,
):
    row, col = lax.axis_index("row"), lax.axis_index("col")
    y, x = row // 2, row % 2
    z, core = col // 2, col % 2
    row_x, row_y = 2 * y + 1 - x, 2 * (1 - y) + x
    x_dev, y_dev = (row_x, col), (row_y, col)
    p_dev = (row, 2 * z + 1 - core)
    z_devs = [(row, 2 * ((z + d) % n_z) + core) for d in range(n_z)]
    rows_u, rows_i = user_in.shape[0], item_in.shape[0]
    size = tile_v.shape[0]
    half, chunk = rows_i // 2, rows_i // 4
    pieces = size // rows_u // 2

    def user_slot(at):
        blocks = size // rows_u
        inner = pl.multiple_of(at % blocks * rows_u, rows_u)
        return u_all.at[at // blocks, pl.ds(inner, rows_u)]

    def item_slot(at, part):
        return i_all.at[at, pl.ds(part * half, half)]

    def copy(src, dst, sends, recvs, at, device):
        return pltpu.make_async_remote_copy(
            src_ref=src,
            dst_ref=dst,
            send_sem=sends.at[at],
            recv_sem=recvs.at[at],
            device_id=device,
            device_id_type=MESH,
        )

    loads = [
        pltpu.make_async_copy(user_in, user_slot(col), load_sem.at[0]),
        pltpu.make_async_copy(item_in, i_all.at[row], load_sem.at[1]),
        pltpu.make_async_copy(tile_in, tile_v, load_sem.at[2]),
    ]
    for load in loads:
        load.start()

    barrier = pltpu.get_barrier_semaphore()
    peers = [x_dev, y_dev, p_dev] + z_devs[1:]
    for peer in peers:
        pl.semaphore_signal(barrier, inc=1, device_id=peer, device_id_type=MESH)
    tu, ti = coords[0], coords[1]
    meta[0] = jnp.full(meta.shape[1:], tu, jnp.int32)
    meta[1] = jnp.full(meta.shape[1:], ti, jnp.int32)
    meta[2] = jnp.full(meta.shape[1:], count[0], jnp.int32)
    my_tu, my_ti, live = meta[0][0:1, :], meta[1][0:1, :], meta[2][0:1, :] > 0
    pl.semaphore_wait(barrier, len(peers))

    sent = []

    def start(c):
        c.start()
        sent.append(c)

    loads[0].wait()
    for d in range(1, n_z):
        start(copy(user_slot(col), user_slot(col), uz_s, uz_r, d, z_devs[d]))
    start(copy(user_slot(col), user_slot(col), up_s, up_r, 0, p_dev))
    loads[1].wait()
    start(copy(item_slot(row, 0), item_slot(row, 0), ig_s, ig_r, 0, x_dev))
    start(copy(item_slot(row, 1), item_slot(row, 1), ig_s, ig_r, 1, y_dev))
    start(copy(item_slot(row, 1), item_slot(row, 1), ig_s, ig_r, 2, x_dev))
    start(copy(item_slot(row, 0), item_slot(row, 0), ig_s, ig_r, 3, y_dev))
    start(copy(meta, meta_x, meta_s, meta_r, 0, x_dev))
    start(copy(meta, meta_y, meta_s, meta_r, 1, y_dev))
    start(copy(meta, meta_p, meta_s, meta_r, 2, p_dev))

    loads[2].wait()
    tile_t[...] = tile_v[...].T

    def arrived(slot, recvs, at):
        copy(slot, slot, recvs, recvs, at, x_dev).wait_recv()

    arrived(item_slot(row_x, 0), ig_r, 0)
    start(copy(item_slot(row_x, 0), item_slot(row_x, 0), ig_s, ig_r, 4, y_dev))
    arrived(item_slot(row_y, 1), ig_r, 1)
    start(copy(item_slot(row_y, 1), item_slot(row_y, 1), ig_s, ig_r, 5, x_dev))
    order = [1] + list(range(n_z - 1, 1, -1)) if n_z > 1 else []
    for d in order:
        slot = user_slot(2 * ((z - d + n_z) % n_z) + core)
        arrived(slot, uz_r, d)
        start(copy(slot, slot, up_s, up_r, d, p_dev))
    for d in [0] + order:
        arrived(user_slot(2 * ((z - d + n_z) % n_z) + 1 - core), up_r, d)

    user_sel = u_all[tu]
    user_sel = jnp.where(live, user_sel, 0.0).astype(user_sel.dtype)
    part_i[...] = jnp.dot(
        tile_t[...], user_sel, preferred_element_type=jnp.float32
    ).reshape(part_i.shape)
    for c in (0, 2, 1, 3):
        start(copy(part_i.at[c], from_1.at[c], r1_s, r1_r, c, x_dev if c < 2 else y_dev))

    diagonal = 2 * (1 - y) + 1 - x
    arrived(item_slot(row_x, 1), ig_r, 2)
    arrived(item_slot(row_y, 0), ig_r, 3)
    arrived(item_slot(diagonal, 0), ig_r, 4)
    arrived(item_slot(diagonal, 1), ig_r, 5)
    item_sel = i_all[ti]
    item_sel = jnp.where(live, item_sel, 0.0).astype(item_sel.dtype)
    part_u[...] = jnp.dot(
        tile_v[...], item_sel, preferred_element_type=jnp.float32
    ).reshape(part_u.shape)
    for h in range(pieces):
        start(copy(part_u.at[2 * h + 1 - core], from_p.at[h], rp_s, rp_r, h, p_dev))

    arrived(meta_x, meta_r, 0)
    arrived(meta_y, meta_r, 1)
    arrived(meta_p, meta_r, 2)

    def second(c):
        other, owner, device = (
            (meta_x, row_y, y_dev) if c < 2 else (meta_y, row_x, x_dev)
        )
        theirs = other[1][0:1, :]
        arrived(from_1.at[c], r1_r, c)
        send_2[c] = jnp.where(my_ti == owner, part_i[c], 0.0) + jnp.where(
            theirs == owner, from_1[c], 0.0
        )
        start(copy(send_2.at[c], from_2.at[c], r2_s, r2_r, c, device))

    second(0)
    second(2)

    partner_tu = meta_p[0][0:1, :]
    for h in range(pieces):
        arrived(from_p.at[h], rp_r, h)
    for d in list(range(1, n_z)) + [0]:
        at = (z + d) % n_z
        tile, h = at // pieces, at % pieces
        send_z[d] = jnp.where(my_tu == tile, part_u[2 * h + core], 0.0) + jnp.where(
            partner_tu == tile, from_p[h], 0.0
        )
        if d:
            start(copy(send_z.at[d], from_z.at[d], rz_s, rz_r, d, z_devs[d]))

    second(1)
    second(3)

    for c in (0, 2, 1, 3):
        theirs = (meta_x if c < 2 else meta_y)[1][0:1, :]
        mine = jnp.where(my_ti == row, part_i[c], 0.0) + jnp.where(theirs == row, from_1[c], 0.0)
        arrived(from_2.at[c], r2_r, c)
        out_i[pl.ds(c * chunk, chunk), :] = (mine + from_2[c]).astype(out_i.dtype)

    total = send_z[0]
    for d in order:
        arrived(from_z.at[d], rz_r, d)
        total = total + from_z[d]
    out_u[...] = total.astype(out_u.dtype)

    for c in sent:
        c.wait_send()


def planned(user_feats, item_feats, tile_values, tile_coords, tile_count, *, n_z):
    rows_u, width = user_feats.shape
    rows_i = item_feats.shape[0]
    size = tile_values.shape[-1]
    f32, bf16, dma = jnp.float32, jnp.bfloat16, pltpu.SemaphoreType.DMA
    blocks = size // rows_u
    vmem = pl.BlockSpec(memory_space=pltpu.VMEM)
    smem = pl.BlockSpec(memory_space=pltpu.SMEM)
    anywhere = pl.BlockSpec(memory_space=pl.ANY)
    quarter = (4, rows_i // 4, width)
    pairs = [3, n_z, n_z, 6, blocks // 2, n_z, 4, 4]
    return pl.pallas_call(
        functools.partial(kernel, n_z),
        out_shape=(
            jax.ShapeDtypeStruct((rows_u, width), bf16),
            jax.ShapeDtypeStruct((rows_i, width), bf16),
        ),
        in_specs=[smem, smem, anywhere, anywhere, anywhere],
        out_specs=(vmem, vmem),
        scratch_shapes=[
            pltpu.VMEM((2 * n_z * rows_u // size, size, width), bf16),
            pltpu.VMEM((4, rows_i, width), bf16),
            pltpu.VMEM((size, size), bf16),
            pltpu.VMEM((size, size), bf16),
            pltpu.VMEM((3, 8, width), jnp.int32),
            pltpu.VMEM((3, 8, width), jnp.int32),
            pltpu.VMEM((3, 8, width), jnp.int32),
            pltpu.VMEM((3, 8, width), jnp.int32),
            pltpu.VMEM((blocks, rows_u, width), f32),
            pltpu.VMEM((blocks // 2, rows_u, width), f32),
            pltpu.VMEM((n_z, rows_u, width), f32),
            pltpu.VMEM((n_z, rows_u, width), f32),
            pltpu.VMEM(quarter, f32),
            pltpu.VMEM(quarter, f32),
            pltpu.VMEM(quarter, f32),
            pltpu.VMEM(quarter, f32),
            dma((3,)),
        ]
        + [dma((n,)) for n in pairs for _ in range(2)],
        compiler_params=pltpu.CompilerParams(collective_id=0, has_side_effects=True),
    )(
        tile_coords.reshape(2),
        tile_count.reshape(1),
        user_feats,
        item_feats,
        tile_values.reshape(size, size),
    )


def solution(mesh):
    n_row, n_col = mesh.shape["row"], mesh.shape["col"]

    def local(user_feats, item_feats, tile_values, tile_coords, tile_count):
        slots, size = tile_values.shape[2], tile_values.shape[3]
        rows_u = user_feats.shape[0]
        fits = (
            n_row == 4
            and n_col % 2 == 0
            and slots == 1
            and item_feats.shape[0] == size
            and size % (2 * rows_u) == 0
            and n_col * rows_u % size == 0
        )
        args = (user_feats, item_feats, tile_values, tile_coords, tile_count)
        return planned(*args, n_z=n_col // 2) if fits else gathered(*args)

    placed = (
        P(("row", "col"), None),
        P(("col", "row"), None),
        P("row", "col", None, None, None),
        P("row", "col", None, None),
        P("row", "col"),
    )
    return jax.shard_map(
        local,
        mesh=mesh,
        in_specs=placed,
        out_specs=(P(("row", "col"), None), P(("col", "row"), None)),
        check_vma=False,
    )
```

```python
import functools

import jax
import jax.numpy as jnp
from jax import lax
from jax.experimental import pallas as pl
from jax.experimental.pallas import tpu as pltpu
from jax.sharding import PartitionSpec as P

MESH = pl.DeviceIdType.MESH


def gathered(user_feats, item_feats, tile_values, tile_coords, tile_count):
    user_block = lax.all_gather(user_feats, "col", axis=0, tiled=True)
    item_block = lax.all_gather(item_feats, "row", axis=0, tiled=True)
    tiles = tile_values[0, 0]
    coords = tile_coords[0, 0]
    count = tile_count[0, 0]
    slots = tiles.shape[0]
    size = tiles.shape[1]
    width = user_block.shape[1]
    user_tiles = user_block.shape[0] // size
    item_tiles = item_block.shape[0] // size
    live = jnp.arange(slots) < count
    pick_user = ((coords[0][:, None] == jnp.arange(user_tiles)[None, :]) & live[:, None]).astype(
        jnp.bfloat16
    )
    pick_item = (coords[1][:, None] == jnp.arange(item_tiles)[None, :]).astype(jnp.bfloat16)
    user_sel = jnp.einsum(
        "su,uiw->siw",
        pick_user,
        user_block.reshape(user_tiles, size, width),
        preferred_element_type=jnp.float32,
    ).astype(jnp.bfloat16)
    item_sel = jnp.einsum(
        "st,tjw->sjw",
        pick_item,
        item_block.reshape(item_tiles, size, width),
        preferred_element_type=jnp.float32,
    ).astype(jnp.bfloat16)
    to_users = jnp.einsum("sij,sjw->siw", tiles, item_sel, preferred_element_type=jnp.float32)
    to_items = jnp.einsum("sij,siw->sjw", tiles, user_sel, preferred_element_type=jnp.float32)
    part_users = jnp.einsum(
        "su,siw->uiw", pick_user.astype(jnp.float32), to_users, precision=lax.Precision.HIGHEST
    ).reshape(user_tiles * size, width)
    part_items = jnp.einsum(
        "st,sjw->tjw", pick_item.astype(jnp.float32), to_items, precision=lax.Precision.HIGHEST
    ).reshape(item_tiles * size, width)
    users_next = lax.psum_scatter(part_users, "col", scatter_dimension=0, tiled=True)
    items_next = lax.psum_scatter(part_items, "row", scatter_dimension=0, tiled=True)
    return (users_next.astype(jnp.bfloat16), items_next.astype(jnp.bfloat16))


def kernel(
    n_z,
    coords,
    count,
    user_in,
    item_in,
    tile_in,
    out_u,
    out_i,
    u_all,
    i_all,
    tile_v,
    tile_t,
    meta,
    meta_x,
    meta_y,
    meta_p,
    part_u,
    from_p,
    send_z,
    from_z,
    part_i,
    from_1,
    send_2,
    from_2,
    load_sem,
    meta_s,
    meta_r,
    uz_s,
    uz_r,
    up_s,
    up_r,
    ig_s,
    ig_r,
    rp_s,
    rp_r,
    rz_s,
    rz_r,
    r1_s,
    r1_r,
    r2_s,
    r2_r,
):
    row, col = lax.axis_index("row"), lax.axis_index("col")
    y, x = row // 2, row % 2
    z, core = col // 2, col % 2
    row_x, row_y = 2 * y + 1 - x, 2 * (1 - y) + x
    x_dev, y_dev = (row_x, col), (row_y, col)
    p_dev = (row, 2 * z + 1 - core)
    z_devs = [(row, 2 * ((z + d) % n_z) + core) for d in range(n_z)]
    rows_u, rows_i = user_in.shape[0], item_in.shape[0]
    size = tile_v.shape[0]
    half, chunk = rows_i // 2, rows_i // 4
    pieces = size // rows_u // 2

    def user_slot(at):
        blocks = size // rows_u
        inner = pl.multiple_of(at % blocks * rows_u, rows_u)
        return u_all.at[at // blocks, pl.ds(inner, rows_u)]

    def item_slot(at, part):
        return i_all.at[at, pl.ds(part * half, half)]

    def copy(src, dst, sends, recvs, at, device):
        return pltpu.make_async_remote_copy(
            src_ref=src,
            dst_ref=dst,
            send_sem=sends.at[at],
            recv_sem=recvs.at[at],
            device_id=device,
            device_id_type=MESH,
        )

    loads = [
        pltpu.make_async_copy(user_in, user_slot(col), load_sem.at[0]),
        pltpu.make_async_copy(item_in, i_all.at[row], load_sem.at[1]),
        pltpu.make_async_copy(tile_in, tile_v, load_sem.at[2]),
    ]
    for load in loads:
        load.start()

    barrier = pltpu.get_barrier_semaphore()
    peers = [x_dev, y_dev, p_dev] + z_devs[1:]
    for peer in peers:
        pl.semaphore_signal(barrier, inc=1, device_id=peer, device_id_type=MESH)
    tu, ti = coords[0], coords[1]
    meta[0] = jnp.full(meta.shape[1:], tu, jnp.int32)
    meta[1] = jnp.full(meta.shape[1:], ti, jnp.int32)
    meta[2] = jnp.full(meta.shape[1:], count[0, 0], jnp.int32)
    my_tu, my_ti, live = meta[0][0:1, :], meta[1][0:1, :], meta[2][0:1, :] > 0
    pl.semaphore_wait(barrier, len(peers))

    sent = []

    def start(c):
        c.start()
        sent.append(c)

    loads[0].wait()
    for d in range(1, n_z):
        start(copy(user_slot(col), user_slot(col), uz_s, uz_r, d, z_devs[d]))
    start(copy(user_slot(col), user_slot(col), up_s, up_r, 0, p_dev))
    loads[1].wait()
    start(copy(item_slot(row, 0), item_slot(row, 0), ig_s, ig_r, 0, x_dev))
    start(copy(item_slot(row, 1), item_slot(row, 1), ig_s, ig_r, 1, y_dev))
    start(copy(item_slot(row, 1), item_slot(row, 1), ig_s, ig_r, 2, x_dev))
    start(copy(item_slot(row, 0), item_slot(row, 0), ig_s, ig_r, 3, y_dev))
    start(copy(meta, meta_x, meta_s, meta_r, 0, x_dev))
    start(copy(meta, meta_y, meta_s, meta_r, 1, y_dev))
    start(copy(meta, meta_p, meta_s, meta_r, 2, p_dev))

    loads[2].wait()
    tile_t[...] = tile_v[...].T

    def arrived(slot, recvs, at):
        copy(slot, slot, recvs, recvs, at, x_dev).wait_recv()

    arrived(item_slot(row_x, 0), ig_r, 0)
    start(copy(item_slot(row_x, 0), item_slot(row_x, 0), ig_s, ig_r, 4, y_dev))
    arrived(item_slot(row_y, 1), ig_r, 1)
    start(copy(item_slot(row_y, 1), item_slot(row_y, 1), ig_s, ig_r, 5, x_dev))
    order = [1] + list(range(n_z - 1, 1, -1)) if n_z > 1 else []
    for d in order:
        slot = user_slot(2 * ((z - d + n_z) % n_z) + core)
        arrived(slot, uz_r, d)
        start(copy(slot, slot, up_s, up_r, d, p_dev))
    for d in [0] + order:
        arrived(user_slot(2 * ((z - d + n_z) % n_z) + 1 - core), up_r, d)

    user_sel = u_all[tu]
    user_sel = jnp.where(live, user_sel, 0.0).astype(user_sel.dtype)
    part_i[...] = jnp.dot(
        tile_t[...], user_sel, preferred_element_type=jnp.float32
    ).reshape(part_i.shape)
    for c in (0, 2, 1, 3):
        start(copy(part_i.at[c], from_1.at[c], r1_s, r1_r, c, x_dev if c < 2 else y_dev))

    diagonal = 2 * (1 - y) + 1 - x
    arrived(item_slot(row_x, 1), ig_r, 2)
    arrived(item_slot(row_y, 0), ig_r, 3)
    arrived(item_slot(diagonal, 0), ig_r, 4)
    arrived(item_slot(diagonal, 1), ig_r, 5)
    item_sel = i_all[ti]
    item_sel = jnp.where(live, item_sel, 0.0).astype(item_sel.dtype)
    part_u[...] = jnp.dot(
        tile_v[...], item_sel, preferred_element_type=jnp.float32
    ).reshape(part_u.shape)
    for h in range(pieces):
        start(copy(part_u.at[2 * h + 1 - core], from_p.at[h], rp_s, rp_r, h, p_dev))

    arrived(meta_x, meta_r, 0)
    arrived(meta_y, meta_r, 1)
    arrived(meta_p, meta_r, 2)

    def second(c):
        other, owner, device = (
            (meta_x, row_y, y_dev) if c < 2 else (meta_y, row_x, x_dev)
        )
        theirs = other[1][0:1, :]
        arrived(from_1.at[c], r1_r, c)
        send_2[c] = jnp.where(my_ti == owner, part_i[c], 0.0) + jnp.where(
            theirs == owner, from_1[c], 0.0
        )
        start(copy(send_2.at[c], from_2.at[c], r2_s, r2_r, c, device))

    partner_tu = meta_p[0][0:1, :]
    for h in range(pieces):
        arrived(from_p.at[h], rp_r, h)
    for d in list(range(1, n_z)) + [0]:
        at = (z + d) % n_z
        tile, h = at // pieces, at % pieces
        send_z[d] = jnp.where(my_tu == tile, part_u[2 * h + core], 0.0) + jnp.where(
            partner_tu == tile, from_p[h], 0.0
        )
        if d:
            start(copy(send_z.at[d], from_z.at[d], rz_s, rz_r, d, z_devs[d]))

    for c in (0, 2, 1, 3):
        second(c)

    for c in (0, 2, 1, 3):
        theirs = (meta_x if c < 2 else meta_y)[1][0:1, :]
        mine = jnp.where(my_ti == row, part_i[c], 0.0) + jnp.where(theirs == row, from_1[c], 0.0)
        arrived(from_2.at[c], r2_r, c)
        out_i[pl.ds(c * chunk, chunk), :] = (mine + from_2[c]).astype(out_i.dtype)

    total = send_z[0]
    for d in order:
        arrived(from_z.at[d], rz_r, d)
        total = total + from_z[d]
    out_u[...] = total.astype(out_u.dtype)

    for c in sent:
        c.wait_send()


def put(users, items, out_u, out_i, sems):
    copies = [
        pltpu.make_async_copy(users, out_u, sems.at[0]),
        pltpu.make_async_copy(items, out_i, sems.at[1]),
    ]
    for c in copies:
        c.start()
    for c in copies:
        c.wait()


def planned(user_feats, item_feats, tile_values, tile_coords, tile_count, *, n_z):
    rows_u, width = user_feats.shape
    rows_i = item_feats.shape[0]
    size = tile_values.shape[-1]
    f32, bf16, dma = jnp.float32, jnp.bfloat16, pltpu.SemaphoreType.DMA
    blocks = size // rows_u
    vmem = pl.BlockSpec(memory_space=pltpu.VMEM)
    smem = pl.BlockSpec(memory_space=pltpu.SMEM)
    anywhere = pl.BlockSpec(memory_space=pl.ANY)
    quarter = (4, rows_i // 4, width)
    pairs = [3, n_z, n_z, 6, blocks // 2, n_z, 4, 4]
    outs = pl.pallas_call(
        functools.partial(kernel, n_z),
        out_shape=(pltpu.VMEM((rows_u, width), bf16), pltpu.VMEM((rows_i, width), bf16)),
        in_specs=[smem, smem, anywhere, anywhere, anywhere],
        out_specs=(vmem, vmem),
        scratch_shapes=[
            pltpu.VMEM((2 * n_z * rows_u // size, size, width), bf16),
            pltpu.VMEM((4, rows_i, width), bf16),
            pltpu.VMEM((size, size), bf16),
            pltpu.VMEM((size, size), bf16),
            pltpu.VMEM((3, 8, width), jnp.int32),
            pltpu.VMEM((3, 8, width), jnp.int32),
            pltpu.VMEM((3, 8, width), jnp.int32),
            pltpu.VMEM((3, 8, width), jnp.int32),
            pltpu.VMEM((blocks, rows_u, width), f32),
            pltpu.VMEM((blocks // 2, rows_u, width), f32),
            pltpu.VMEM((n_z, rows_u, width), f32),
            pltpu.VMEM((n_z, rows_u, width), f32),
            pltpu.VMEM(quarter, f32),
            pltpu.VMEM(quarter, f32),
            pltpu.VMEM(quarter, f32),
            pltpu.VMEM(quarter, f32),
            dma((3,)),
        ]
        + [dma((n,)) for n in pairs for _ in range(2)],
        compiler_params=pltpu.CompilerParams(collective_id=0, has_side_effects=True),
    )(
        tile_coords.reshape(2),
        tile_count,
        user_feats,
        item_feats,
        tile_values.reshape(size, size),
    )
    return pl.pallas_call(
        put,
        out_shape=[jax.ShapeDtypeStruct(out.shape, out.dtype) for out in outs],
        in_specs=[vmem, vmem],
        out_specs=[anywhere, anywhere],
        scratch_shapes=[dma((2,))],
    )(*[pltpu.with_memory_space_constraint(out, pltpu.VMEM) for out in outs])


def solution(mesh):
    n_row, n_col = mesh.shape["row"], mesh.shape["col"]

    def local(user_feats, item_feats, tile_values, tile_coords, tile_count):
        slots, size = tile_values.shape[2], tile_values.shape[3]
        rows_u = user_feats.shape[0]
        fits = (
            n_row == 4
            and n_col % 2 == 0
            and slots == 1
            and item_feats.shape[0] == size
            and size % (2 * rows_u) == 0
            and n_col * rows_u % size == 0
        )
        args = (user_feats, item_feats, tile_values, tile_coords, tile_count)
        return planned(*args, n_z=n_col // 2) if fits else gathered(*args)

    placed = (
        P(("row", "col"), None),
        P(("col", "row"), None),
        P("row", "col", None, None, None),
        P("row", "col", None, None),
        P("row", "col"),
    )
    return jax.shard_map(
        local,
        mesh=mesh,
        in_specs=placed,
        out_specs=(P(("row", "col"), None), P(("col", "row"), None)),
        check_vma=False,
    )
```

```python
import functools

import jax
import jax.numpy as jnp
from jax import lax
from jax.experimental import pallas as pl
from jax.experimental.pallas import tpu as pltpu
from jax.sharding import PartitionSpec as P

MESH = pl.DeviceIdType.MESH


def gathered(user_feats, item_feats, tile_values, tile_coords, tile_count):
    user_block = lax.all_gather(user_feats, "col", axis=0, tiled=True)
    item_block = lax.all_gather(item_feats, "row", axis=0, tiled=True)
    tiles = tile_values[0, 0]
    coords = tile_coords[0, 0]
    count = tile_count[0, 0]
    slots = tiles.shape[0]
    size = tiles.shape[1]
    width = user_block.shape[1]
    user_tiles = user_block.shape[0] // size
    item_tiles = item_block.shape[0] // size
    live = jnp.arange(slots) < count
    pick_user = ((coords[0][:, None] == jnp.arange(user_tiles)[None, :]) & live[:, None]).astype(
        jnp.bfloat16
    )
    pick_item = (coords[1][:, None] == jnp.arange(item_tiles)[None, :]).astype(jnp.bfloat16)
    user_sel = jnp.einsum(
        "su,uiw->siw",
        pick_user,
        user_block.reshape(user_tiles, size, width),
        preferred_element_type=jnp.float32,
    ).astype(jnp.bfloat16)
    item_sel = jnp.einsum(
        "st,tjw->sjw",
        pick_item,
        item_block.reshape(item_tiles, size, width),
        preferred_element_type=jnp.float32,
    ).astype(jnp.bfloat16)
    to_users = jnp.einsum("sij,sjw->siw", tiles, item_sel, preferred_element_type=jnp.float32)
    to_items = jnp.einsum("sij,siw->sjw", tiles, user_sel, preferred_element_type=jnp.float32)
    part_users = jnp.einsum(
        "su,siw->uiw", pick_user.astype(jnp.float32), to_users, precision=lax.Precision.HIGHEST
    ).reshape(user_tiles * size, width)
    part_items = jnp.einsum(
        "st,sjw->tjw", pick_item.astype(jnp.float32), to_items, precision=lax.Precision.HIGHEST
    ).reshape(item_tiles * size, width)
    users_next = lax.psum_scatter(part_users, "col", scatter_dimension=0, tiled=True)
    items_next = lax.psum_scatter(part_items, "row", scatter_dimension=0, tiled=True)
    return (users_next.astype(jnp.bfloat16), items_next.astype(jnp.bfloat16))


def kernel(
    n_z,
    coords_in,
    count_in,
    user_in,
    item_in,
    tile_in,
    out_u,
    out_i,
    u_all,
    i_all,
    tile_v,
    tile_t,
    meta,
    meta_x,
    meta_y,
    meta_p,
    part_u,
    from_p,
    send_z,
    from_z,
    part_i,
    from_1,
    send_2,
    from_2,
    coords,
    count,
    load_sem,
    meta_s,
    meta_r,
    uz_s,
    uz_r,
    up_s,
    up_r,
    ig_s,
    ig_r,
    rp_s,
    rp_r,
    rz_s,
    rz_r,
    r1_s,
    r1_r,
    r2_s,
    r2_r,
):
    row, col = lax.axis_index("row"), lax.axis_index("col")
    y, x = row // 2, row % 2
    z, core = col // 2, col % 2
    row_x, row_y = 2 * y + 1 - x, 2 * (1 - y) + x
    x_dev, y_dev = (row_x, col), (row_y, col)
    p_dev = (row, 2 * z + 1 - core)

    def far_first(at):
        flip = z // (n_z // 2)
        mirrored = z + flip * (n_z - 1 - 2 * z)
        to = n_z - 1 - at
        to = jnp.where(to <= mirrored, to - 1, to)
        return to + flip * (n_z - 1 - 2 * to)

    others = [far_first(at) for at in range(n_z - 1)]
    z_devs = [(row, 2 * at + core) for at in others]
    near_first = others[::-1]
    rows_u, rows_i = user_in.shape[0], item_in.shape[0]
    size = tile_v.shape[0]
    half, chunk = rows_i // 2, rows_i // 4
    pieces = size // rows_u // 2

    def user_slot(at):
        blocks = size // rows_u
        inner = pl.multiple_of(at % blocks * rows_u, rows_u)
        return u_all.at[at // blocks, pl.ds(inner, rows_u)]

    def item_slot(at, part):
        return i_all.at[at, pl.ds(part * half, half)]

    def copy(src, dst, sends, recvs, at, device, to=None):
        return pltpu.make_async_remote_copy(
            src_ref=src,
            dst_ref=dst,
            send_sem=sends.at[at if to is None else to],
            recv_sem=recvs.at[at],
            device_id=device,
            device_id_type=MESH,
        )

    barrier = pltpu.get_barrier_semaphore()
    peers = [x_dev, y_dev, p_dev] + z_devs
    for peer in peers:
        pl.semaphore_signal(barrier, inc=1, device_id=peer, device_id_type=MESH)
    loads = [
        pltpu.make_async_copy(user_in, user_slot(col), load_sem.at[0]),
        pltpu.make_async_copy(item_in, i_all.at[row], load_sem.at[1]),
        pltpu.make_async_copy(tile_in, tile_v, load_sem.at[2]),
        pltpu.make_async_copy(coords_in, coords, load_sem.at[3]),
        pltpu.make_async_copy(count_in, count, load_sem.at[4]),
    ]
    for load in loads:
        load.start()

    loads[3].wait()
    loads[4].wait()
    tu, ti = coords[0], coords[1]
    meta[0] = jnp.full(meta.shape[1:], tu, jnp.int32)
    meta[1] = jnp.full(meta.shape[1:], ti, jnp.int32)
    meta[2] = jnp.full(meta.shape[1:], count[0, 0], jnp.int32)
    my_tu, my_ti, live = meta[0][0:1, :], meta[1][0:1, :], meta[2][0:1, :] > 0
    pl.semaphore_wait(barrier, len(peers))

    sent = []

    def start(c):
        c.start()
        sent.append(c)

    loads[0].wait()
    for to, device in zip(others, z_devs):
        start(copy(user_slot(col), user_slot(col), uz_s, uz_r, z, device, to))
    start(copy(user_slot(col), user_slot(col), up_s, up_r, z, p_dev))
    loads[1].wait()
    start(copy(item_slot(row, 0), item_slot(row, 0), ig_s, ig_r, 0, x_dev))
    start(copy(item_slot(row, 1), item_slot(row, 1), ig_s, ig_r, 1, y_dev))
    start(copy(item_slot(row, 1), item_slot(row, 1), ig_s, ig_r, 2, x_dev))
    start(copy(item_slot(row, 0), item_slot(row, 0), ig_s, ig_r, 3, y_dev))
    start(copy(meta, meta_x, meta_s, meta_r, 0, x_dev))
    start(copy(meta, meta_y, meta_s, meta_r, 1, y_dev))
    start(copy(meta, meta_p, meta_s, meta_r, 2, p_dev))

    loads[2].wait()
    tile_t[...] = tile_v[...].T

    def arrived(slot, recvs, at):
        copy(slot, slot, recvs, recvs, at, x_dev).wait_recv()

    arrived(item_slot(row_x, 0), ig_r, 0)
    start(copy(item_slot(row_x, 0), item_slot(row_x, 0), ig_s, ig_r, 4, y_dev))
    arrived(item_slot(row_y, 1), ig_r, 1)
    start(copy(item_slot(row_y, 1), item_slot(row_y, 1), ig_s, ig_r, 5, x_dev))
    for at in near_first:
        slot = user_slot(2 * at + core)
        arrived(slot, uz_r, at)
        start(copy(slot, slot, up_s, up_r, at, p_dev))
    for at in [z] + near_first:
        arrived(user_slot(2 * at + 1 - core), up_r, at)

    user_sel = u_all[tu]
    user_sel = jnp.where(live, user_sel, 0.0).astype(user_sel.dtype)
    part_i[...] = jnp.dot(
        tile_t[...], user_sel, preferred_element_type=jnp.float32
    ).reshape(part_i.shape)
    for c in (0, 2, 1, 3):
        start(copy(part_i.at[c], from_1.at[c], r1_s, r1_r, c, x_dev if c < 2 else y_dev))

    diagonal = 2 * (1 - y) + 1 - x
    arrived(item_slot(row_x, 1), ig_r, 2)
    arrived(item_slot(row_y, 0), ig_r, 3)
    arrived(item_slot(diagonal, 0), ig_r, 4)
    arrived(item_slot(diagonal, 1), ig_r, 5)
    item_sel = i_all[ti]
    item_sel = jnp.where(live, item_sel, 0.0).astype(item_sel.dtype)
    part_u[...] = jnp.dot(
        tile_v[...], item_sel, preferred_element_type=jnp.float32
    ).reshape(part_u.shape)
    for h in range(pieces):
        start(copy(part_u.at[2 * h + 1 - core], from_p.at[h], rp_s, rp_r, h, p_dev))

    arrived(meta_x, meta_r, 0)
    arrived(meta_y, meta_r, 1)
    arrived(meta_p, meta_r, 2)

    def second(c):
        other, owner, device = (
            (meta_x, row_y, y_dev) if c < 2 else (meta_y, row_x, x_dev)
        )
        theirs = other[1][0:1, :]
        arrived(from_1.at[c], r1_r, c)
        send_2[c] = jnp.where(my_ti == owner, part_i[c], 0.0) + jnp.where(
            theirs == owner, from_1[c], 0.0
        )
        start(copy(send_2.at[c], from_2.at[c], r2_s, r2_r, c, device))

    partner_tu = meta_p[0][0:1, :]
    for h in range(pieces):
        arrived(from_p.at[h], rp_r, h)
    for at, device in list(zip(others, z_devs)) + [(z, None)]:
        tile, h = at // pieces, at % pieces
        send_z[at] = jnp.where(my_tu == tile, part_u[2 * h + core], 0.0) + jnp.where(
            partner_tu == tile, from_p[h], 0.0
        )
        if device is not None:
            start(copy(send_z.at[at], from_z.at[z], rz_s, rz_r, z, device, at))

    for c in (0, 2, 1, 3):
        second(c)

    for c in (0, 2, 1, 3):
        theirs = (meta_x if c < 2 else meta_y)[1][0:1, :]
        mine = jnp.where(my_ti == row, part_i[c], 0.0) + jnp.where(theirs == row, from_1[c], 0.0)
        arrived(from_2.at[c], r2_r, c)
        out_i[pl.ds(c * chunk, chunk), :] = (mine + from_2[c]).astype(out_i.dtype)

    total = send_z[z]
    for at in near_first:
        arrived(from_z.at[at], rz_r, at)
        total = total + from_z[at]
    out_u[...] = total.astype(out_u.dtype)

    for c in sent:
        c.wait_send()


def put(users, items, out_u, out_i, sems):
    copies = [
        pltpu.make_async_copy(users, out_u, sems.at[0]),
        pltpu.make_async_copy(items, out_i, sems.at[1]),
    ]
    for c in copies:
        c.start()
    for c in copies:
        c.wait()


def planned(user_feats, item_feats, tile_values, tile_coords, tile_count, *, n_z):
    rows_u, width = user_feats.shape
    rows_i = item_feats.shape[0]
    size = tile_values.shape[-1]
    f32, bf16, dma = jnp.float32, jnp.bfloat16, pltpu.SemaphoreType.DMA
    blocks = size // rows_u
    vmem = pl.BlockSpec(memory_space=pltpu.VMEM)
    anywhere = pl.BlockSpec(memory_space=pl.ANY)
    quarter = (4, rows_i // 4, width)
    pairs = [3, n_z, n_z, 6, blocks // 2, n_z, 4, 4]
    outs = pl.pallas_call(
        functools.partial(kernel, n_z),
        out_shape=(pltpu.VMEM((rows_u, width), bf16), pltpu.VMEM((rows_i, width), bf16)),
        in_specs=[anywhere] * 5,
        out_specs=(vmem, vmem),
        scratch_shapes=[
            pltpu.VMEM((2 * n_z * rows_u // size, size, width), bf16),
            pltpu.VMEM((4, rows_i, width), bf16),
            pltpu.VMEM((size, size), bf16),
            pltpu.VMEM((size, size), bf16),
            pltpu.VMEM((3, 8, width), jnp.int32),
            pltpu.VMEM((3, 8, width), jnp.int32),
            pltpu.VMEM((3, 8, width), jnp.int32),
            pltpu.VMEM((3, 8, width), jnp.int32),
            pltpu.VMEM((blocks, rows_u, width), f32),
            pltpu.VMEM((blocks // 2, rows_u, width), f32),
            pltpu.VMEM((n_z, rows_u, width), f32),
            pltpu.VMEM((n_z, rows_u, width), f32),
            pltpu.VMEM(quarter, f32),
            pltpu.VMEM(quarter, f32),
            pltpu.VMEM(quarter, f32),
            pltpu.VMEM(quarter, f32),
            pltpu.SMEM((2,), jnp.int32),
            pltpu.SMEM((1, 1), jnp.int32),
            dma((5,)),
        ]
        + [dma((n,)) for n in pairs for _ in range(2)],
        compiler_params=pltpu.CompilerParams(collective_id=0, has_side_effects=True),
    )(
        tile_coords.reshape(2),
        tile_count,
        user_feats,
        item_feats,
        tile_values.reshape(size, size),
    )
    return pl.pallas_call(
        put,
        out_shape=[jax.ShapeDtypeStruct(out.shape, out.dtype) for out in outs],
        in_specs=[vmem, vmem],
        out_specs=[anywhere, anywhere],
        scratch_shapes=[dma((2,))],
    )(*[pltpu.with_memory_space_constraint(out, pltpu.VMEM) for out in outs])


def solution(mesh):
    n_row, n_col = mesh.shape["row"], mesh.shape["col"]

    def local(user_feats, item_feats, tile_values, tile_coords, tile_count):
        slots, size = tile_values.shape[2], tile_values.shape[3]
        rows_u = user_feats.shape[0]
        fits = (
            n_row == 4
            and n_col % 2 == 0
            and slots == 1
            and item_feats.shape[0] == size
            and size % (2 * rows_u) == 0
            and n_col * rows_u % size == 0
        )
        args = (user_feats, item_feats, tile_values, tile_coords, tile_count)
        return planned(*args, n_z=n_col // 2) if fits else gathered(*args)

    placed = (
        P(("row", "col"), None),
        P(("col", "row"), None),
        P("row", "col", None, None, None),
        P("row", "col", None, None),
        P("row", "col"),
    )
    return jax.shard_map(
        local,
        mesh=mesh,
        in_specs=placed,
        out_specs=(P(("row", "col"), None), P(("col", "row"), None)),
        check_vma=False,
    )
```

```python
import functools

import jax
import jax.numpy as jnp
from jax import lax
from jax.experimental import pallas as pl
from jax.experimental.pallas import tpu as pltpu
from jax.sharding import PartitionSpec as P

MESH = pl.DeviceIdType.MESH


def gathered(user_feats, item_feats, tile_values, tile_coords, tile_count):
    user_block = lax.all_gather(user_feats, "col", axis=0, tiled=True)
    item_block = lax.all_gather(item_feats, "row", axis=0, tiled=True)
    tiles = tile_values[0, 0]
    coords = tile_coords[0, 0]
    count = tile_count[0, 0]
    slots = tiles.shape[0]
    size = tiles.shape[1]
    width = user_block.shape[1]
    user_tiles = user_block.shape[0] // size
    item_tiles = item_block.shape[0] // size
    live = jnp.arange(slots) < count
    pick_user = ((coords[0][:, None] == jnp.arange(user_tiles)[None, :]) & live[:, None]).astype(
        jnp.bfloat16
    )
    pick_item = (coords[1][:, None] == jnp.arange(item_tiles)[None, :]).astype(jnp.bfloat16)
    user_sel = jnp.einsum(
        "su,uiw->siw",
        pick_user,
        user_block.reshape(user_tiles, size, width),
        preferred_element_type=jnp.float32,
    ).astype(jnp.bfloat16)
    item_sel = jnp.einsum(
        "st,tjw->sjw",
        pick_item,
        item_block.reshape(item_tiles, size, width),
        preferred_element_type=jnp.float32,
    ).astype(jnp.bfloat16)
    to_users = jnp.einsum("sij,sjw->siw", tiles, item_sel, preferred_element_type=jnp.float32)
    to_items = jnp.einsum("sij,siw->sjw", tiles, user_sel, preferred_element_type=jnp.float32)
    part_users = jnp.einsum(
        "su,siw->uiw", pick_user.astype(jnp.float32), to_users, precision=lax.Precision.HIGHEST
    ).reshape(user_tiles * size, width)
    part_items = jnp.einsum(
        "st,sjw->tjw", pick_item.astype(jnp.float32), to_items, precision=lax.Precision.HIGHEST
    ).reshape(item_tiles * size, width)
    users_next = lax.psum_scatter(part_users, "col", scatter_dimension=0, tiled=True)
    items_next = lax.psum_scatter(part_items, "row", scatter_dimension=0, tiled=True)
    return (users_next.astype(jnp.bfloat16), items_next.astype(jnp.bfloat16))


def kernel(
    n_z,
    coords_in,
    count_in,
    user_in,
    item_in,
    tile_in,
    out_u,
    out_i,
    u_all,
    i_all,
    tile_v,
    tile_t,
    meta,
    metas,
    part_u,
    from_p,
    send_z,
    from_z,
    part_i,
    from_1,
    send_2,
    from_2,
    coords,
    count,
    load_sem,
    meta_s,
    meta_r,
    uz_s,
    uz_r,
    up_s,
    up_r,
    ig_s,
    ig_r,
    rp_s,
    rp_r,
    rz_s,
    rz_r,
    r1_s,
    r1_r,
    r2_s,
    r2_r,
):
    row, col = lax.axis_index("row"), lax.axis_index("col")
    y, x = row // 2, row % 2
    z, core = col // 2, col % 2
    row_x, row_y = 2 * y + 1 - x, 2 * (1 - y) + x
    x_dev, y_dev = (row_x, col), (row_y, col)
    p_dev = (row, 2 * z + 1 - core)

    def far_first(at):
        flip = z // (n_z // 2)
        mirrored = z + flip * (n_z - 1 - 2 * z)
        to = n_z - 1 - at
        to = jnp.where(to <= mirrored, to - 1, to)
        return to + flip * (n_z - 1 - 2 * to)

    others = [far_first(at) for at in range(n_z - 1)]
    z_devs = [(row, 2 * at + core) for at in others]
    near_first = others[::-1]
    rows_u, rows_i = user_in.shape[0], item_in.shape[0]
    size = tile_v.shape[-1]
    chunk = rows_i // 4
    pieces = size // rows_u // 2

    def user_slot(at):
        blocks = size // rows_u
        inner = pl.multiple_of(at % blocks * rows_u, rows_u)
        return u_all.at[at // blocks, pl.ds(inner, rows_u)]

    def item_slot(at, part, parts=2):
        rows = rows_i // parts
        return i_all.at[at, pl.ds(part * rows, rows)]

    def copy(src, dst, send, recv, device):
        return pltpu.make_async_remote_copy(
            src_ref=src,
            dst_ref=dst,
            send_sem=send,
            recv_sem=recv,
            device_id=device,
            device_id_type=MESH,
        )

    def arrived(like, recv):
        copy(like, like, recv, recv, x_dev).wait_recv()

    def left(like, send):
        copy(like, like, send, send, x_dev).wait_send()

    barrier = pltpu.get_barrier_semaphore()
    peers = [x_dev, y_dev, p_dev] + z_devs
    for peer in peers:
        pl.semaphore_signal(barrier, inc=1, device_id=peer, device_id_type=MESH)
    loads = [
        pltpu.make_async_copy(user_in, user_slot(col), load_sem.at[0]),
        pltpu.make_async_copy(item_in, i_all.at[row], load_sem.at[1]),
        pltpu.make_async_copy(tile_in, tile_v, load_sem.at[2]),
        pltpu.make_async_copy(coords_in, coords, load_sem.at[3]),
        pltpu.make_async_copy(count_in, count, load_sem.at[4]),
    ]
    for load in loads:
        load.start()

    loads[3].wait()
    loads[4].wait()
    tu, ti = coords[0], coords[1]
    meta[0] = jnp.full(meta.shape[1:], tu, jnp.int32)
    meta[1] = jnp.full(meta.shape[1:], ti, jnp.int32)
    meta[2] = jnp.full(meta.shape[1:], count[0, 0], jnp.int32)
    my_tu, my_ti, live = meta[0][0:1, :], meta[1][0:1, :], meta[2][0:1, :] > 0
    pl.semaphore_wait(barrier, len(peers))

    def relay_item(at, part, recv, device):
        piece = item_slot(at, part, 4)
        copy(piece, piece, ig_s.at[0], ig_r.at[recv], device).start()

    loads[0].wait()
    own = user_slot(col)
    for device in z_devs:
        copy(own, own, uz_s.at[0], uz_r.at[z], device).start()
    copy(own, own, up_s.at[0], up_r.at[0], p_dev).start()
    loads[1].wait()
    for part in range(2):
        relay_item(row, part, part, x_dev)
        relay_item(row, 2 + part, 2 + part, y_dev)
    for part, device in ((1, x_dev), (0, y_dev)):
        piece = item_slot(row, part)
        copy(piece, piece, ig_s.at[0], ig_r.at[4], device).start()
    for at, device in enumerate((x_dev, y_dev, p_dev)):
        copy(meta, metas.at[at], meta_s.at[0], meta_r.at[0], device).start()
    meta_x, meta_y, meta_p = metas.at[0], metas.at[1], metas.at[2]

    loads[2].wait()
    tile_t[...] = tile_v[...].reshape(size, size).T

    for part in range(2):
        arrived(item_slot(row_x, part, 4), ig_r.at[part])
        relay_item(row_x, part, 4, y_dev)
        arrived(item_slot(row_y, 2 + part, 4), ig_r.at[2 + part])
        relay_item(row_y, 2 + part, 4, x_dev)
    for at in near_first:
        slot = user_slot(2 * at + core)
        arrived(slot, uz_r.at[at])
        copy(slot, slot, up_s.at[0], up_r.at[0], p_dev).start()
    half_users = u_all.at[pl.ds(0, u_all.shape[0] // 2)]
    arrived(half_users, up_r.at[0])

    user_sel = u_all[tu]
    user_sel = jnp.where(live, user_sel, 0.0).astype(user_sel.dtype)
    part_i[...] = jnp.dot(
        tile_t[...], user_sel, preferred_element_type=jnp.float32
    ).reshape(part_i.shape)
    for c in (0, 2, 1, 3):
        copy(
            part_i.at[c], from_1.at[c], r1_s.at[0], r1_r.at[c], x_dev if c < 2 else y_dev
        ).start()

    arrived(i_all.at[pl.ds(0, 2)], ig_r.at[4])
    item_sel = i_all[ti]
    item_sel = jnp.where(live, item_sel, 0.0).astype(item_sel.dtype)

    def multiply(b):
        part_u[b] = jnp.dot(tile_v[b], item_sel, preferred_element_type=jnp.float32)

    for h in range(pieces):
        multiply(2 * h + 1 - core)
        copy(part_u.at[2 * h + 1 - core], from_p.at[h], rp_s.at[0], rp_r.at[0], p_dev).start()
    for h in range(pieces):
        multiply(2 * h + core)
    arrived(metas, meta_r.at[0])

    def second(c):
        other, owner, device = (
            (meta_x, row_y, y_dev) if c < 2 else (meta_y, row_x, x_dev)
        )
        theirs = other[1][0:1, :]
        arrived(from_1.at[c], r1_r.at[c])
        send_2[c] = jnp.where(my_ti == owner, part_i[c], 0.0) + jnp.where(
            theirs == owner, from_1[c], 0.0
        )
        copy(send_2.at[c], from_2.at[c], r2_s.at[0], r2_r.at[c], device).start()

    partner_tu = meta_p[0][0:1, :]
    arrived(from_p, rp_r.at[0])
    for at, device in list(zip(others, z_devs)) + [(z, None)]:
        tile, h = at // pieces, at % pieces
        send_z[at] = jnp.where(my_tu == tile, part_u[2 * h + core], 0.0) + jnp.where(
            partner_tu == tile, from_p[h], 0.0
        )
        if device is not None:
            copy(send_z.at[at], from_z.at[z], rz_s.at[0], rz_r.at[0], device).start()

    for c in (0, 2, 1, 3):
        second(c)

    for c in (0, 2, 1, 3):
        theirs = (meta_x if c < 2 else meta_y)[1][0:1, :]
        mine = jnp.where(my_ti == row, part_i[c], 0.0) + jnp.where(theirs == row, from_1[c], 0.0)
        arrived(from_2.at[c], r2_r.at[c])
        out_i[pl.ds(c * chunk, chunk), :] = (mine + from_2[c]).astype(out_i.dtype)

    total = send_z[z]
    arrived(from_z.at[pl.ds(0, n_z - 1)], rz_r.at[0])
    for at in near_first:
        total = total + from_z[at]
    out_u[...] = total.astype(out_u.dtype)

    left(u_all.at[0, pl.ds(0, (n_z - 1) * rows_u)], uz_s.at[0])
    left(half_users, up_s.at[0])
    left(i_all.at[pl.ds(0, 3)], ig_s.at[0])
    left(metas, meta_s.at[0])
    left(part_i, r1_s.at[0])
    left(from_p, rp_s.at[0])
    left(send_2, r2_s.at[0])
    left(send_z.at[pl.ds(0, n_z - 1)], rz_s.at[0])


def put(users, items, out_u, out_i, sems):
    copies = [
        pltpu.make_async_copy(users, out_u, sems.at[0]),
        pltpu.make_async_copy(items, out_i, sems.at[1]),
    ]
    for c in copies:
        c.start()
    for c in copies:
        c.wait()


def planned(user_feats, item_feats, tile_values, tile_coords, tile_count, *, n_z):
    rows_u, width = user_feats.shape
    rows_i = item_feats.shape[0]
    size = tile_values.shape[-1]
    f32, bf16, dma = jnp.float32, jnp.bfloat16, pltpu.SemaphoreType.DMA
    blocks = size // rows_u
    vmem = pl.BlockSpec(memory_space=pltpu.VMEM)
    anywhere = pl.BlockSpec(memory_space=pl.ANY)
    quarter = (4, rows_i // 4, width)
    arrivals = [1, n_z, 1, 5, 1, 1, 4, 4]
    outs = pl.pallas_call(
        functools.partial(kernel, n_z),
        out_shape=(pltpu.VMEM((rows_u, width), bf16), pltpu.VMEM((rows_i, width), bf16)),
        in_specs=[anywhere] * 5,
        out_specs=(vmem, vmem),
        scratch_shapes=[
            pltpu.VMEM((2 * n_z * rows_u // size, size, width), bf16),
            pltpu.VMEM((4, rows_i, width), bf16),
            pltpu.VMEM((blocks, rows_u, size), bf16),
            pltpu.VMEM((size, size), bf16),
            pltpu.VMEM((3, 8, width), jnp.int32),
            pltpu.VMEM((3, 3, 8, width), jnp.int32),
            pltpu.VMEM((blocks, rows_u, width), f32),
            pltpu.VMEM((blocks // 2, rows_u, width), f32),
            pltpu.VMEM((n_z, rows_u, width), f32),
            pltpu.VMEM((n_z, rows_u, width), f32),
            pltpu.VMEM(quarter, f32),
            pltpu.VMEM(quarter, f32),
            pltpu.VMEM(quarter, f32),
            pltpu.VMEM(quarter, f32),
            pltpu.SMEM((2,), jnp.int32),
            pltpu.SMEM((1, 1), jnp.int32),
            dma((5,)),
        ]
        + [dma((n,)) for arrival in arrivals for n in (1, arrival)],
        compiler_params=pltpu.CompilerParams(collective_id=0, has_side_effects=True),
    )(
        tile_coords.reshape(2),
        tile_count,
        user_feats,
        item_feats,
        tile_values.reshape(blocks, rows_u, size),
    )
    return pl.pallas_call(
        put,
        out_shape=[jax.ShapeDtypeStruct(out.shape, out.dtype) for out in outs],
        in_specs=[vmem, vmem],
        out_specs=[anywhere, anywhere],
        scratch_shapes=[dma((2,))],
    )(*[pltpu.with_memory_space_constraint(out, pltpu.VMEM) for out in outs])


def solution(mesh):
    n_row, n_col = mesh.shape["row"], mesh.shape["col"]

    def local(user_feats, item_feats, tile_values, tile_coords, tile_count):
        slots, size = tile_values.shape[2], tile_values.shape[3]
        rows_u = user_feats.shape[0]
        fits = (
            n_row == 4
            and n_col % 2 == 0
            and slots == 1
            and item_feats.shape[0] == size
            and size % (2 * rows_u) == 0
            and n_col * rows_u % (2 * size) == 0
            and (n_col // 2 - 1) * rows_u <= size
        )
        args = (user_feats, item_feats, tile_values, tile_coords, tile_count)
        return planned(*args, n_z=n_col // 2) if fits else gathered(*args)

    placed = (
        P(("row", "col"), None),
        P(("col", "row"), None),
        P("row", "col", None, None, None),
        P("row", "col", None, None),
        P("row", "col"),
    )
    return jax.shard_map(
        local,
        mesh=mesh,
        in_specs=placed,
        out_specs=(P(("row", "col"), None), P(("col", "row"), None)),
        check_vma=False,
    )
```

```python
import functools

import jax
import jax.numpy as jnp
from jax import lax
from jax.experimental import pallas as pl
from jax.experimental.pallas import tpu as pltpu
from jax.sharding import PartitionSpec as P

MESH = pl.DeviceIdType.MESH


def gathered(user_feats, item_feats, tile_values, tile_coords, tile_count):
    user_block = lax.all_gather(user_feats, "col", axis=0, tiled=True)
    item_block = lax.all_gather(item_feats, "row", axis=0, tiled=True)
    tiles = tile_values[0, 0]
    coords = tile_coords[0, 0]
    count = tile_count[0, 0]
    slots = tiles.shape[0]
    size = tiles.shape[1]
    width = user_block.shape[1]
    user_tiles = user_block.shape[0] // size
    item_tiles = item_block.shape[0] // size
    live = jnp.arange(slots) < count
    pick_user = ((coords[0][:, None] == jnp.arange(user_tiles)[None, :]) & live[:, None]).astype(
        jnp.bfloat16
    )
    pick_item = (coords[1][:, None] == jnp.arange(item_tiles)[None, :]).astype(jnp.bfloat16)
    user_sel = jnp.einsum(
        "su,uiw->siw",
        pick_user,
        user_block.reshape(user_tiles, size, width),
        preferred_element_type=jnp.float32,
    ).astype(jnp.bfloat16)
    item_sel = jnp.einsum(
        "st,tjw->sjw",
        pick_item,
        item_block.reshape(item_tiles, size, width),
        preferred_element_type=jnp.float32,
    ).astype(jnp.bfloat16)
    to_users = jnp.einsum("sij,sjw->siw", tiles, item_sel, preferred_element_type=jnp.float32)
    to_items = jnp.einsum("sij,siw->sjw", tiles, user_sel, preferred_element_type=jnp.float32)
    part_users = jnp.einsum(
        "su,siw->uiw", pick_user.astype(jnp.float32), to_users, precision=lax.Precision.HIGHEST
    ).reshape(user_tiles * size, width)
    part_items = jnp.einsum(
        "st,sjw->tjw", pick_item.astype(jnp.float32), to_items, precision=lax.Precision.HIGHEST
    ).reshape(item_tiles * size, width)
    users_next = lax.psum_scatter(part_users, "col", scatter_dimension=0, tiled=True)
    items_next = lax.psum_scatter(part_items, "row", scatter_dimension=0, tiled=True)
    return (users_next.astype(jnp.bfloat16), items_next.astype(jnp.bfloat16))


def kernel(
    n_z,
    coords_in,
    count_in,
    user_in,
    item_in,
    tile_in,
    out_u,
    out_i,
    u_all,
    i_all,
    tile_v,
    tile_t,
    meta,
    metas,
    part_u,
    from_p,
    send_z,
    from_z,
    via,
    part_i,
    from_1,
    send_2,
    from_2,
    coords,
    count,
    load_sem,
    via_r,
    meta_s,
    meta_r,
    uz_s,
    uz_r,
    up_s,
    up_r,
    ig_s,
    ig_r,
    rp_s,
    rp_r,
    rz_s,
    rz_r,
    r1_s,
    r1_r,
    r2_s,
    r2_r,
):
    row, col = lax.axis_index("row"), lax.axis_index("col")
    y, x = row // 2, row % 2
    z, core = col // 2, col % 2
    row_x, row_y = 2 * y + 1 - x, 2 * (1 - y) + x
    x_dev, y_dev = (row_x, col), (row_y, col)
    p_dev = (row, 2 * z + 1 - core)

    def far_first(at):
        flip = z // (n_z // 2)
        mirrored = z + flip * (n_z - 1 - 2 * z)
        to = n_z - 1 - at
        to = jnp.where(to <= mirrored, to - 1, to)
        return to + flip * (n_z - 1 - 2 * to)

    others = [far_first(at) for at in range(n_z - 1)]
    z_devs = [(row, 2 * at + core) for at in others]
    near_first = others[::-1]
    flip = z // 2
    far, cross, beside = 3 - 3 * flip, 2 - flip, z + 1 - 2 * (z % 2)
    edge = z % 3 == 0
    rows_u, rows_i = user_in.shape[0], item_in.shape[0]
    size = tile_v.shape[-1]
    chunk = rows_i // 4
    pieces = size // rows_u // 2

    def user_slot(at):
        blocks = size // rows_u
        inner = pl.multiple_of(at % blocks * rows_u, rows_u)
        return u_all.at[at // blocks, pl.ds(inner, rows_u)]

    def item_slot(at, part, parts=2):
        rows = rows_i // parts
        return i_all.at[at, pl.ds(part * rows, rows)]

    def copy(src, dst, send, recv, device):
        return pltpu.make_async_remote_copy(
            src_ref=src,
            dst_ref=dst,
            send_sem=send,
            recv_sem=recv,
            device_id=device,
            device_id_type=MESH,
        )

    def arrived(like, recv):
        copy(like, like, recv, recv, x_dev).wait_recv()

    def left(like, send):
        copy(like, like, send, send, x_dev).wait_send()

    barrier = pltpu.get_barrier_semaphore()
    peers = [x_dev, y_dev, p_dev] + z_devs
    for peer in peers:
        pl.semaphore_signal(barrier, inc=1, device_id=peer, device_id_type=MESH)
    loads = [
        pltpu.make_async_copy(user_in, user_slot(col), load_sem.at[0]),
        pltpu.make_async_copy(item_in, i_all.at[row], load_sem.at[1]),
        pltpu.make_async_copy(tile_in, tile_v, load_sem.at[2]),
        pltpu.make_async_copy(coords_in, coords, load_sem.at[3]),
        pltpu.make_async_copy(count_in, count, load_sem.at[4]),
    ]
    for load in loads:
        load.start()

    loads[3].wait()
    loads[4].wait()
    tu, ti = coords[0], coords[1]
    meta[0] = jnp.full(meta.shape[1:], tu, jnp.int32)
    meta[1] = jnp.full(meta.shape[1:], ti, jnp.int32)
    meta[2] = jnp.full(meta.shape[1:], count[0, 0], jnp.int32)
    my_tu, my_ti, live = meta[0][0:1, :], meta[1][0:1, :], meta[2][0:1, :] > 0
    pl.semaphore_wait(barrier, len(peers))

    def relay_item(at, part, recv, device):
        piece = item_slot(at, part, 4)
        copy(piece, piece, ig_s.at[0], ig_r.at[recv], device).start()

    loads[0].wait()
    own = user_slot(col)
    for device in z_devs:
        copy(own, own, uz_s.at[0], uz_r.at[z], device).start()
    copy(own, own, up_s.at[0], up_r.at[0], p_dev).start()
    loads[1].wait()
    for part in range(2):
        relay_item(row, part, part, x_dev)
        relay_item(row, 2 + part, 2 + part, y_dev)
    for part, device in ((1, x_dev), (0, y_dev)):
        piece = item_slot(row, part)
        copy(piece, piece, ig_s.at[0], ig_r.at[4], device).start()
    for at, device in enumerate((x_dev, y_dev, p_dev)):
        copy(meta, metas.at[at], meta_s.at[0], meta_r.at[0], device).start()
    meta_x, meta_y, meta_p = metas.at[0], metas.at[1], metas.at[2]

    loads[2].wait()
    tile_t[...] = tile_v[...].reshape(size, size).T

    for part in range(2):
        arrived(item_slot(row_x, part, 4), ig_r.at[part])
        relay_item(row_x, part, 4, y_dev)
        arrived(item_slot(row_y, 2 + part, 4), ig_r.at[2 + part])
        relay_item(row_y, 2 + part, 4, x_dev)
    for at in near_first:
        slot = user_slot(2 * at + core)
        arrived(slot, uz_r.at[at])
        copy(slot, slot, up_s.at[0], up_r.at[0], p_dev).start()
    half_users = u_all.at[pl.ds(0, u_all.shape[0] // 2)]
    arrived(half_users, up_r.at[0])

    user_sel = u_all[tu]
    user_sel = jnp.where(live, user_sel, 0.0).astype(user_sel.dtype)
    part_i[...] = jnp.dot(
        tile_t[...], user_sel, preferred_element_type=jnp.float32
    ).reshape(part_i.shape)
    for c in (0, 2, 1, 3):
        copy(
            part_i.at[c], from_1.at[c], r1_s.at[0], r1_r.at[c], x_dev if c < 2 else y_dev
        ).start()

    arrived(i_all.at[pl.ds(0, 2)], ig_r.at[4])
    item_sel = i_all[ti]
    item_sel = jnp.where(live, item_sel, 0.0).astype(item_sel.dtype)

    def multiply(owner):
        rows = jnp.concatenate([tile_v[2 * h + owner] for h in range(pieces)], axis=0)
        product = jnp.dot(rows, item_sel, preferred_element_type=jnp.float32)
        for h in range(pieces):
            part_u[2 * h + owner] = product[h * rows_u : (h + 1) * rows_u]

    multiply(1 - core)
    for h in range(pieces):
        copy(part_u.at[2 * h + 1 - core], from_p.at[h], rp_s.at[0], rp_r.at[0], p_dev).start()
    multiply(core)
    arrived(metas, meta_r.at[0])

    def second(c):
        other, owner, device = (
            (meta_x, row_y, y_dev) if c < 2 else (meta_y, row_x, x_dev)
        )
        theirs = other[1][0:1, :]
        arrived(from_1.at[c], r1_r.at[c])
        send_2[c] = jnp.where(my_ti == owner, part_i[c], 0.0) + jnp.where(
            theirs == owner, from_1[c], 0.0
        )
        copy(send_2.at[c], from_2.at[c], r2_s.at[0], r2_r.at[c], device).start()

    partner_tu = meta_p[0][0:1, :]
    arrived(from_p, rp_r.at[0])

    def combine(at):
        tile, h = at // pieces, at % pieces
        send_z[at] = jnp.where(my_tu == tile, part_u[2 * h + core], 0.0) + jnp.where(
            partner_tu == tile, from_p[h], 0.0
        )

    def along_z(at, dst, recv, to):
        device = (row, 2 * to + core)
        copy(send_z.at[at], dst, rz_s.at[0], recv, device).start()

    combine(cross)

    @pl.when(edge)
    def _():
        along_z(cross, via, via_r.at[0], beside)

    for at in (far, beside):
        combine(at)
        along_z(at, from_z.at[z], rz_r.at[0], at)
    combine(z)

    for c in (0, 2, 1, 3):
        second(c)

    @pl.when(jnp.logical_not(edge))
    def _():
        arrived(via, via_r.at[0])
        send_z[cross] = send_z[cross] + via[...]
        along_z(cross, from_z.at[z], rz_r.at[0], cross)

    for c in (0, 2, 1, 3):
        theirs = (meta_x if c < 2 else meta_y)[1][0:1, :]
        mine = jnp.where(my_ti == row, part_i[c], 0.0) + jnp.where(theirs == row, from_1[c], 0.0)
        arrived(from_2.at[c], r2_r.at[c])
        out_i[pl.ds(c * chunk, chunk), :] = (mine + from_2[c]).astype(out_i.dtype)

    def finish(sources):
        arrived(from_z.at[pl.ds(0, len(sources))], rz_r.at[0])
        total = send_z[z]
        for at in sources:
            total = total + from_z[at]
        out_u[...] = total.astype(out_u.dtype)

    @pl.when(edge)
    def _():
        finish([beside, cross, far])

    @pl.when(jnp.logical_not(edge))
    def _():
        finish([beside, cross])

    left(u_all.at[0, pl.ds(0, (n_z - 1) * rows_u)], uz_s.at[0])
    left(half_users, up_s.at[0])
    left(i_all.at[pl.ds(0, 3)], ig_s.at[0])
    left(metas, meta_s.at[0])
    left(part_i, r1_s.at[0])
    left(from_p, rp_s.at[0])
    left(send_2, r2_s.at[0])
    left(send_z.at[pl.ds(0, n_z - 1)], rz_s.at[0])


def put(users, items, out_u, out_i, sems):
    copies = [
        pltpu.make_async_copy(users, out_u, sems.at[0]),
        pltpu.make_async_copy(items, out_i, sems.at[1]),
    ]
    for c in copies:
        c.start()
    for c in copies:
        c.wait()


def planned(user_feats, item_feats, tile_values, tile_coords, tile_count, *, n_z):
    rows_u, width = user_feats.shape
    rows_i = item_feats.shape[0]
    size = tile_values.shape[-1]
    f32, bf16, dma = jnp.float32, jnp.bfloat16, pltpu.SemaphoreType.DMA
    blocks = size // rows_u
    vmem = pl.BlockSpec(memory_space=pltpu.VMEM)
    anywhere = pl.BlockSpec(memory_space=pl.ANY)
    quarter = (4, rows_i // 4, width)
    arrivals = [1, n_z, 1, 5, 1, 1, 4, 4]
    outs = pl.pallas_call(
        functools.partial(kernel, n_z),
        out_shape=(pltpu.VMEM((rows_u, width), bf16), pltpu.VMEM((rows_i, width), bf16)),
        in_specs=[anywhere] * 5,
        out_specs=(vmem, vmem),
        scratch_shapes=[
            pltpu.VMEM((2 * n_z * rows_u // size, size, width), bf16),
            pltpu.VMEM((4, rows_i, width), bf16),
            pltpu.VMEM((blocks, rows_u, size), bf16),
            pltpu.VMEM((size, size), bf16),
            pltpu.VMEM((3, 8, width), jnp.int32),
            pltpu.VMEM((3, 3, 8, width), jnp.int32),
            pltpu.VMEM((blocks, rows_u, width), f32),
            pltpu.VMEM((blocks // 2, rows_u, width), f32),
            pltpu.VMEM((n_z, rows_u, width), f32),
            pltpu.VMEM((n_z, rows_u, width), f32),
            pltpu.VMEM((rows_u, width), f32),
            pltpu.VMEM(quarter, f32),
            pltpu.VMEM(quarter, f32),
            pltpu.VMEM(quarter, f32),
            pltpu.VMEM(quarter, f32),
            pltpu.SMEM((2,), jnp.int32),
            pltpu.SMEM((1, 1), jnp.int32),
            dma((5,)),
            dma((1,)),
        ]
        + [dma((n,)) for arrival in arrivals for n in (1, arrival)],
        compiler_params=pltpu.CompilerParams(collective_id=0, has_side_effects=True),
    )(
        tile_coords.reshape(2),
        tile_count,
        user_feats,
        item_feats,
        tile_values.reshape(blocks, rows_u, size),
    )
    return pl.pallas_call(
        put,
        out_shape=[jax.ShapeDtypeStruct(out.shape, out.dtype) for out in outs],
        in_specs=[vmem, vmem],
        out_specs=[anywhere, anywhere],
        scratch_shapes=[dma((2,))],
    )(*[pltpu.with_memory_space_constraint(out, pltpu.VMEM) for out in outs])


def solution(mesh):
    n_row, n_col = mesh.shape["row"], mesh.shape["col"]

    def local(user_feats, item_feats, tile_values, tile_coords, tile_count):
        slots, size = tile_values.shape[2], tile_values.shape[3]
        rows_u = user_feats.shape[0]
        fits = (
            n_row == 4
            and n_col == 8
            and slots == 1
            and item_feats.shape[0] == size
            and size % (2 * rows_u) == 0
            and n_col * rows_u % (2 * size) == 0
            and (n_col // 2 - 1) * rows_u <= size
        )
        args = (user_feats, item_feats, tile_values, tile_coords, tile_count)
        return planned(*args, n_z=n_col // 2) if fits else gathered(*args)

    placed = (
        P(("row", "col"), None),
        P(("col", "row"), None),
        P("row", "col", None, None, None),
        P("row", "col", None, None),
        P("row", "col"),
    )
    return jax.shard_map(
        local,
        mesh=mesh,
        in_specs=placed,
        out_specs=(P(("row", "col"), None), P(("col", "row"), None)),
        check_vma=False,
    )
```

```python
import functools

import jax
import jax.numpy as jnp
from jax import lax
from jax.experimental import pallas as pl
from jax.experimental.pallas import tpu as pltpu
from jax.sharding import PartitionSpec as P

MESH = pl.DeviceIdType.MESH


def gathered(user_feats, item_feats, tile_values, tile_coords, tile_count):
    user_block = lax.all_gather(user_feats, "col", axis=0, tiled=True)
    item_block = lax.all_gather(item_feats, "row", axis=0, tiled=True)
    tiles = tile_values[0, 0]
    coords = tile_coords[0, 0]
    count = tile_count[0, 0]
    slots = tiles.shape[0]
    size = tiles.shape[1]
    width = user_block.shape[1]
    user_tiles = user_block.shape[0] // size
    item_tiles = item_block.shape[0] // size
    live = jnp.arange(slots) < count
    pick_user = ((coords[0][:, None] == jnp.arange(user_tiles)[None, :]) & live[:, None]).astype(
        jnp.bfloat16
    )
    pick_item = (coords[1][:, None] == jnp.arange(item_tiles)[None, :]).astype(jnp.bfloat16)
    user_sel = jnp.einsum(
        "su,uiw->siw",
        pick_user,
        user_block.reshape(user_tiles, size, width),
        preferred_element_type=jnp.float32,
    ).astype(jnp.bfloat16)
    item_sel = jnp.einsum(
        "st,tjw->sjw",
        pick_item,
        item_block.reshape(item_tiles, size, width),
        preferred_element_type=jnp.float32,
    ).astype(jnp.bfloat16)
    to_users = jnp.einsum("sij,sjw->siw", tiles, item_sel, preferred_element_type=jnp.float32)
    to_items = jnp.einsum("sij,siw->sjw", tiles, user_sel, preferred_element_type=jnp.float32)
    part_users = jnp.einsum(
        "su,siw->uiw", pick_user.astype(jnp.float32), to_users, precision=lax.Precision.HIGHEST
    ).reshape(user_tiles * size, width)
    part_items = jnp.einsum(
        "st,sjw->tjw", pick_item.astype(jnp.float32), to_items, precision=lax.Precision.HIGHEST
    ).reshape(item_tiles * size, width)
    users_next = lax.psum_scatter(part_users, "col", scatter_dimension=0, tiled=True)
    items_next = lax.psum_scatter(part_items, "row", scatter_dimension=0, tiled=True)
    return (users_next.astype(jnp.bfloat16), items_next.astype(jnp.bfloat16))


def kernel(
    n_z,
    coords_in,
    count_in,
    user_in,
    item_in,
    tile_in,
    out_u,
    out_i,
    u_all,
    i_all,
    tile_v,
    tile_t,
    meta,
    metas,
    part_u,
    from_p,
    send_z,
    from_z,
    part_i,
    from_1,
    send_2,
    from_2,
    coords,
    count,
    load_sem,
    meta_s,
    meta_r,
    uz_s,
    uz_r,
    up_s,
    up_r,
    ig_s,
    ig_r,
    rp_s,
    rp_r,
    rz_s,
    rz_r,
    r1_s,
    r1_r,
    r2_s,
    r2_r,
):
    row, col = lax.axis_index("row"), lax.axis_index("col")
    y, x = row // 2, row % 2
    z, core = col // 2, col % 2
    row_x, row_y = 2 * y + 1 - x, 2 * (1 - y) + x
    x_dev, y_dev = (row_x, col), (row_y, col)
    p_dev = (row, 2 * z + 1 - core)

    def far_first(at):
        flip = z // (n_z // 2)
        mirrored = z + flip * (n_z - 1 - 2 * z)
        to = n_z - 1 - at
        to = jnp.where(to <= mirrored, to - 1, to)
        return to + flip * (n_z - 1 - 2 * to)

    others = [far_first(at) for at in range(n_z - 1)]
    z_devs = [(row, 2 * at + core) for at in others]
    near_first = others[::-1]
    rows_u, rows_i = user_in.shape[0], item_in.shape[0]
    size = tile_v.shape[-1]
    chunk = rows_i // 4
    pieces = size // rows_u // 2

    def user_slot(at):
        blocks = size // rows_u
        inner = pl.multiple_of(at % blocks * rows_u, rows_u)
        return u_all.at[at // blocks, pl.ds(inner, rows_u)]

    def item_slot(at, part, parts=2):
        rows = rows_i // parts
        return i_all.at[at, pl.ds(part * rows, rows)]

    def copy(src, dst, send, recv, device):
        return pltpu.make_async_remote_copy(
            src_ref=src,
            dst_ref=dst,
            send_sem=send,
            recv_sem=recv,
            device_id=device,
            device_id_type=MESH,
        )

    def arrived(like, recv):
        copy(like, like, recv, recv, x_dev).wait_recv()

    def left(like, send):
        copy(like, like, send, send, x_dev).wait_send()

    barrier = pltpu.get_barrier_semaphore()
    peers = [x_dev, y_dev, p_dev] + z_devs
    for peer in peers:
        pl.semaphore_signal(barrier, inc=1, device_id=peer, device_id_type=MESH)
    loads = [
        pltpu.make_async_copy(user_in, user_slot(col), load_sem.at[0]),
        pltpu.make_async_copy(item_in, i_all.at[row], load_sem.at[1]),
        pltpu.make_async_copy(tile_in, tile_v, load_sem.at[2]),
        pltpu.make_async_copy(coords_in, coords, load_sem.at[3]),
        pltpu.make_async_copy(count_in, count, load_sem.at[4]),
    ]
    for load in loads:
        load.start()

    loads[3].wait()
    loads[4].wait()
    tu, ti = coords[0], coords[1]
    meta[0] = jnp.full(meta.shape[1:], tu, jnp.int32)
    meta[1] = jnp.full(meta.shape[1:], ti, jnp.int32)
    meta[2] = jnp.full(meta.shape[1:], count[0, 0], jnp.int32)
    my_tu, my_ti, live = meta[0][0:1, :], meta[1][0:1, :], meta[2][0:1, :] > 0
    pl.semaphore_wait(barrier, len(peers))

    def relay_item(at, part, recv, device):
        piece = item_slot(at, part, 4)
        copy(piece, piece, ig_s.at[0], ig_r.at[recv], device).start()

    loads[0].wait()
    own = user_slot(col)
    for device in z_devs:
        copy(own, own, uz_s.at[0], uz_r.at[z], device).start()
    copy(own, own, up_s.at[0], up_r.at[0], p_dev).start()
    loads[1].wait()
    for part in range(2):
        relay_item(row, part, part, x_dev)
        relay_item(row, 2 + part, 2 + part, y_dev)
    for part, device in ((1, x_dev), (0, y_dev)):
        piece = item_slot(row, part)
        copy(piece, piece, ig_s.at[0], ig_r.at[4], device).start()
    for at, device in enumerate((x_dev, y_dev, p_dev)):
        copy(meta, metas.at[at], meta_s.at[0], meta_r.at[0], device).start()
    meta_x, meta_y, meta_p = metas.at[0], metas.at[1], metas.at[2]

    loads[2].wait()
    tile_t[...] = tile_v[...].reshape(size, size).T

    for part in range(2):
        arrived(item_slot(row_x, part, 4), ig_r.at[part])
        relay_item(row_x, part, 4, y_dev)
        arrived(item_slot(row_y, 2 + part, 4), ig_r.at[2 + part])
        relay_item(row_y, 2 + part, 4, x_dev)
    for at in near_first:
        slot = user_slot(2 * at + core)
        arrived(slot, uz_r.at[at])
        copy(slot, slot, up_s.at[0], up_r.at[0], p_dev).start()
    half_users = u_all.at[pl.ds(0, u_all.shape[0] // 2)]
    arrived(half_users, up_r.at[0])

    user_sel = u_all[tu]
    user_sel = jnp.where(live, user_sel, 0.0).astype(user_sel.dtype)
    part_i[...] = jnp.dot(
        tile_t[...], user_sel, preferred_element_type=jnp.float32
    ).reshape(part_i.shape)
    for c in (0, 2, 1, 3):
        copy(
            part_i.at[c], from_1.at[c], r1_s.at[0], r1_r.at[c], x_dev if c < 2 else y_dev
        ).start()

    arrived(i_all.at[pl.ds(0, 2)], ig_r.at[4])
    item_sel = i_all[ti]
    item_sel = jnp.where(live, item_sel, 0.0).astype(item_sel.dtype)

    def multiply(owner):
        rows = jnp.concatenate([tile_v[2 * h + owner] for h in range(pieces)], axis=0)
        product = jnp.dot(rows, item_sel, preferred_element_type=jnp.float32)
        for h in range(pieces):
            part_u[2 * h + owner] = product[h * rows_u : (h + 1) * rows_u]

    multiply(1 - core)
    for h in range(pieces):
        copy(part_u.at[2 * h + 1 - core], from_p.at[h], rp_s.at[0], rp_r.at[0], p_dev).start()
    multiply(core)
    arrived(metas, meta_r.at[0])

    def second(c):
        other, owner, device = (
            (meta_x, row_y, y_dev) if c < 2 else (meta_y, row_x, x_dev)
        )
        theirs = other[1][0:1, :]
        arrived(from_1.at[c], r1_r.at[c])
        send_2[c] = jnp.where(my_ti == owner, part_i[c], 0.0) + jnp.where(
            theirs == owner, from_1[c], 0.0
        )
        copy(send_2.at[c], from_2.at[c], r2_s.at[0], r2_r.at[c], device).start()

    partner_tu = meta_p[0][0:1, :]
    arrived(from_p, rp_r.at[0])
    for at, device in list(zip(others, z_devs)) + [(z, None)]:
        tile, h = at // pieces, at % pieces
        send_z[at] = jnp.where(my_tu == tile, part_u[2 * h + core], 0.0) + jnp.where(
            partner_tu == tile, from_p[h], 0.0
        )
        if device is not None:
            copy(send_z.at[at], from_z.at[z], rz_s.at[0], rz_r.at[0], device).start()

    for c in (0, 2, 1, 3):
        second(c)

    for c in (0, 2, 1, 3):
        theirs = (meta_x if c < 2 else meta_y)[1][0:1, :]
        mine = jnp.where(my_ti == row, part_i[c], 0.0) + jnp.where(theirs == row, from_1[c], 0.0)
        arrived(from_2.at[c], r2_r.at[c])
        out_i[pl.ds(c * chunk, chunk), :] = (mine + from_2[c]).astype(out_i.dtype)

    total = send_z[z]
    arrived(from_z.at[pl.ds(0, n_z - 1)], rz_r.at[0])
    for at in near_first:
        total = total + from_z[at]
    out_u[...] = total.astype(out_u.dtype)

    left(u_all.at[0, pl.ds(0, (n_z - 1) * rows_u)], uz_s.at[0])
    left(half_users, up_s.at[0])
    left(i_all.at[pl.ds(0, 3)], ig_s.at[0])
    left(metas, meta_s.at[0])
    left(part_i, r1_s.at[0])
    left(from_p, rp_s.at[0])
    left(send_2, r2_s.at[0])
    left(send_z.at[pl.ds(0, n_z - 1)], rz_s.at[0])


def put(users, items, out_u, out_i, sems):
    copies = [
        pltpu.make_async_copy(users, out_u, sems.at[0]),
        pltpu.make_async_copy(items, out_i, sems.at[1]),
    ]
    for c in copies:
        c.start()
    for c in copies:
        c.wait()


def planned(user_feats, item_feats, tile_values, tile_coords, tile_count, *, n_z):
    rows_u, width = user_feats.shape
    rows_i = item_feats.shape[0]
    size = tile_values.shape[-1]
    f32, bf16, dma = jnp.float32, jnp.bfloat16, pltpu.SemaphoreType.DMA
    blocks = size // rows_u
    vmem = pl.BlockSpec(memory_space=pltpu.VMEM)
    anywhere = pl.BlockSpec(memory_space=pl.ANY)
    quarter = (4, rows_i // 4, width)
    arrivals = [1, n_z, 1, 5, 1, 1, 4, 4]
    outs = pl.pallas_call(
        functools.partial(kernel, n_z),
        out_shape=(pltpu.VMEM((rows_u, width), bf16), pltpu.VMEM((rows_i, width), bf16)),
        in_specs=[anywhere] * 5,
        out_specs=(vmem, vmem),
        scratch_shapes=[
            pltpu.VMEM((2 * n_z * rows_u // size, size, width), bf16),
            pltpu.VMEM((4, rows_i, width), bf16),
            pltpu.VMEM((blocks, rows_u, size), bf16),
            pltpu.VMEM((size, size), bf16),
            pltpu.VMEM((3, 8, width), jnp.int32),
            pltpu.VMEM((3, 3, 8, width), jnp.int32),
            pltpu.VMEM((blocks, rows_u, width), f32),
            pltpu.VMEM((blocks // 2, rows_u, width), f32),
            pltpu.VMEM((n_z, rows_u, width), f32),
            pltpu.VMEM((n_z, rows_u, width), f32),
            pltpu.VMEM(quarter, f32),
            pltpu.VMEM(quarter, f32),
            pltpu.VMEM(quarter, f32),
            pltpu.VMEM(quarter, f32),
            pltpu.SMEM((2,), jnp.int32),
            pltpu.SMEM((1, 1), jnp.int32),
            dma((5,)),
        ]
        + [dma((n,)) for arrival in arrivals for n in (1, arrival)],
        compiler_params=pltpu.CompilerParams(collective_id=0, has_side_effects=True),
    )(
        tile_coords.reshape(2),
        tile_count,
        user_feats,
        item_feats,
        tile_values.reshape(blocks, rows_u, size),
    )
    return pl.pallas_call(
        put,
        out_shape=[jax.ShapeDtypeStruct(out.shape, out.dtype) for out in outs],
        in_specs=[vmem, vmem],
        out_specs=[anywhere, anywhere],
        scratch_shapes=[dma((2,))],
    )(*[pltpu.with_memory_space_constraint(out, pltpu.VMEM) for out in outs])


def solution(mesh):
    n_row, n_col = mesh.shape["row"], mesh.shape["col"]

    def local(user_feats, item_feats, tile_values, tile_coords, tile_count):
        slots, size = tile_values.shape[2], tile_values.shape[3]
        rows_u = user_feats.shape[0]
        fits = (
            n_row == 4
            and n_col % 2 == 0
            and slots == 1
            and item_feats.shape[0] == size
            and size % (2 * rows_u) == 0
            and n_col * rows_u % (2 * size) == 0
            and (n_col // 2 - 1) * rows_u <= size
        )
        args = (user_feats, item_feats, tile_values, tile_coords, tile_count)
        return planned(*args, n_z=n_col // 2) if fits else gathered(*args)

    placed = (
        P(("row", "col"), None),
        P(("col", "row"), None),
        P("row", "col", None, None, None),
        P("row", "col", None, None),
        P("row", "col"),
    )
    return jax.shard_map(
        local,
        mesh=mesh,
        in_specs=placed,
        out_specs=(P(("row", "col"), None), P(("col", "row"), None)),
        check_vma=False,
    )
```
